32 devices in a mesh: pix: 8 (over z, y), rep: 4 (over x, core).
Axes of the slice: x: 2, y: 2, z: 4, core: 2. Of those that a mesh axis runs over, the one named last changes fastest.
Arguments:
- interferograms: float32 [256, 131072], P(('pix', 'rep')), may hold values from -6 to 6
- epoch_pairs: int32 [2, 256], replicated, may hold values from 0 to 63, as said below
- los: float32 [3, 131072], P(None, ('pix', 'rep')), may hold values from 0.3 to 1
- patch_place: int32 [2, 4096], replicated, may hold values from 0 to 255, as said below
- patch_depth: int32 [4096], replicated, may hold values from 0 to 7
Outputs:
- predicted: float32 [64, 131072], P(None, ('pix', 'rep'))
- slip: float32 [64, 4096], P(None, ('pix', 'rep'))
The draws below stay inside these ranges and needn't reach their ends.
Inputs may be any that keep to these rules, and one draw needn't show every extreme that they name: `epoch_pairs`: row 0 holds an interferogram's earlier epoch and row 1 its later one; the two always differ. `patch_place`: row 0 is an east cell below 256; row 1 is a north cell below 32.
All inputs are finite; a program needn't handle non-finite values.
Results may differ from the reference program's by a relative error of at most 0.0037.
Values may be sent and summed in bfloat16 or wider, within the bound.
A program may use at most 64 MiB of HBM per device.

```python
import jax
import jax.numpy as jnp
from jax import lax

NEP = 64
NIFG = 256
NPATCH = 4096
IMG_W = 1024
SWEEPS = 2
PIX_DEV = 4096
NPIX = 131072
DEVICES = 32


def draw_epoch_pairs(key, part):
    first_key = jax.random.fold_in(key, 11)
    span_key = jax.random.fold_in(key, 12)
    primary = jax.random.randint(first_key, (NIFG,), 0, NEP - 1)
    spread = jax.random.randint(span_key, (NIFG,), 0, 1 << 20)
    secondary = primary + 1 + spread % (NEP - 1 - primary)
    return jnp.stack([primary, secondary]).astype(jnp.int32)


def draw_patch_place(key, part):
    north_cells = max(NPIX // (4 * IMG_W), 1)
    east = jax.random.randint(jax.random.fold_in(key, 31), (NPATCH,), 0, 256)
    north = jax.random.randint(jax.random.fold_in(key, 32), (NPATCH,), 0, north_cells)
    return jnp.stack([east, north]).astype(jnp.int32)


def draw_los(key, part):
    return jax.random.uniform(jax.random.fold_in(key, 41), (3, NPIX), jnp.float32, 0.3, 1.0)


def touch_ends(result, rng, least, high):
    shape = result.shape
    spot = [jax.random.randint(jax.random.fold_in(rng, axis), (), 0, shape[axis]) for axis in range(len(shape))]
    result = result.at[tuple(spot)].set(least)
    longest = shape.index(max(shape))
    spot[longest] = (spot[longest] + 1) % shape[longest]
    return result.at[tuple(spot)].set(high)


def level_of(rng, dims, split, least, high):
    level = 1.0
    for position, parts in split:
        draws = jax.random.uniform(jax.random.fold_in(jax.random.fold_in(rng, 6), position), (parts,), jnp.float32, least / len(split), high / len(split))
        level = level * jnp.repeat(jnp.exp(draws), dims[position] // parts).reshape((-1,) + (1,) * (len(dims) - 1 - position))
    return level


def centred(stream_key, shape, width, limit, cuts=(), kind=jnp.bfloat16):
    level = level_of(stream_key, shape, cuts, -0.22, 0.18) if cuts else 1.0
    values = jax.random.normal(stream_key, shape, jnp.float32) * width * level
    return jnp.minimum(jnp.maximum(values, -limit), limit).astype(kind)


def setup_inputs(seed: int = 0) -> dict:
    streams_of = jax.random.split(jax.random.key(seed), 6)
    return {
        "interferograms": centred(streams_of[0], (NIFG, NPIX), 1.0, 6.0, ((0, 32),), jnp.float32),
        "epoch_pairs": draw_epoch_pairs(jax.random.fold_in(streams_of[5], 71), 0),
        "los": draw_los(jax.random.fold_in(streams_of[5], 71), 0),
        "patch_place": draw_patch_place(jax.random.fold_in(streams_of[5], 71), 0),
        "patch_depth": touch_ends(jax.random.randint(streams_of[4], (NPATCH,), 0, 8), jax.random.fold_in(streams_of[4], 1), 0, 7).astype(jnp.int32),
    }


pixel_step = 0.1
patch_step = 0.4
damping = 0.5
depth_base = 0.5
depth_step = 0.25

def sbas_inverse(epoch_pairs):
    epochs = lax.iota(jnp.int32, NEP)
    design = (epochs[None, :] == epoch_pairs[1][:, None]).astype(jnp.float32) - (epochs[None, :] == epoch_pairs[0][:, None]).astype(jnp.float32)
    normal = jnp.dot(design.T, design, precision=lax.Precision.HIGHEST) + damping * jnp.eye(NEP, dtype=jnp.float32)
    factor = jnp.linalg.cholesky(normal)
    return jax.scipy.linalg.cho_solve((factor, True), design.T)

def green_tile(pixel, los_rows, patch_place, patch_depth):
    column = (pixel % IMG_W).astype(jnp.float32)
    line = (pixel // IMG_W).astype(jnp.float32)
    xpos = (column + 0.5) * pixel_step
    ypos = (line + 0.5) * pixel_step
    patch_x = (patch_place[0].astype(jnp.float32) + 0.5) * patch_step
    patch_y = (patch_place[1].astype(jnp.float32) + 0.5) * patch_step
    patch_z = depth_base + depth_step * patch_depth.astype(jnp.float32)
    delta_x = xpos[:, None] - patch_x[None, :]
    delta_y = ypos[:, None] - patch_y[None, :]
    delta_z = patch_z[None, :]
    dist_sq = delta_x * delta_x + delta_y * delta_y + delta_z * delta_z
    toward = los_rows[0][:, None] * delta_x + los_rows[1][:, None] * delta_y + los_rows[2][:, None] * delta_z
    return (delta_z * toward / (dist_sq * jnp.sqrt(dist_sq))).astype(jnp.bfloat16)

def reference(interferograms, epoch_pairs, los, patch_place, patch_depth):
    pseudo = sbas_inverse(epoch_pairs)
    series = jnp.dot(pseudo.astype(jnp.float32), interferograms.astype(jnp.float32), precision=lax.Precision.HIGHEST, preferred_element_type=jnp.float32)
    total = PIX_DEV * DEVICES
    blocks = total // PIX_DEV
    indices = jnp.arange(blocks, dtype=jnp.int32)

    def tile_at(index):
        start = index * PIX_DEV
        pixel = start + lax.iota(jnp.int32, PIX_DEV)
        los_rows = lax.dynamic_slice_in_dim(los, start, PIX_DEV, 1)
        return (green_tile(pixel, los_rows, patch_place, patch_depth), start)

    def first_step(carry, index):
        rhs, bound = carry
        tile, start = tile_at(index)
        resid = lax.dynamic_slice_in_dim(series, start, PIX_DEV, 1).astype(jnp.bfloat16)
        rhs = rhs + jnp.dot(resid.astype(jnp.float32), tile.astype(jnp.float32), preferred_element_type=jnp.float32)
        magnitude = jnp.abs(tile)
        weight = lax.optimization_barrier(jnp.sum(magnitude.astype(jnp.float32), axis=1)).astype(jnp.bfloat16)
        bound = bound + jnp.dot(weight[None, :].astype(jnp.float32), magnitude.astype(jnp.float32), preferred_element_type=jnp.float32)[0]
        return ((rhs, bound), None)
    zero_rhs = jnp.zeros((NEP, NPATCH), jnp.float32)
    zero_bound = jnp.zeros((NPATCH,), jnp.float32)
    (rhs, bound), unused = lax.scan(first_step, (zero_rhs, zero_bound), indices)
    slip = jnp.zeros((NEP, NPATCH), jnp.float32) + rhs / bound[None, :]
    for sweep in range(1, SWEEPS):
        slip_half = slip.astype(jnp.bfloat16)

        def sweep_step(rhs_now, index):
            tile, start = tile_at(index)
            guess = lax.dot_general(slip_half.astype(jnp.float32), tile.astype(jnp.float32), (((1,), (1,)), ((), ())), preferred_element_type=jnp.float32)
            resid = (lax.dynamic_slice_in_dim(series, start, PIX_DEV, 1) - guess).astype(jnp.bfloat16)
            return (rhs_now + jnp.dot(resid.astype(jnp.float32), tile.astype(jnp.float32), preferred_element_type=jnp.float32), None)
        rhs, unused = lax.scan(sweep_step, zero_rhs, indices)
        slip = slip + rhs / bound[None, :]
    slip_half = slip.astype(jnp.bfloat16)

    def final_block(index):
        tile, start = tile_at(index)
        return lax.dot_general(slip_half.astype(jnp.float32), tile.astype(jnp.float32), (((1,), (1,)), ((), ())), preferred_element_type=jnp.float32)
    pieces = lax.map(final_block, indices)
    predicted = jnp.transpose(pieces, (1, 0, 2)).reshape(NEP, total)
    return (predicted, slip)
```

```python
import functools

import jax
import jax.numpy as jnp
from jax import lax
from jax.experimental import pallas as pl
from jax.experimental.pallas import tpu as pltpu
from jax.sharding import PartitionSpec as P

NEP = 64
IMG_W = 1024
LANES = 128

pixel_step = 0.1
patch_step = 0.4
damping = 0.5
depth_base = 0.5
depth_step = 0.25

F32 = jnp.float32
BF16 = jnp.bfloat16
NT = (((1,), (1,)), ((), ()))
EXTRA = 16


def kernel(
    cfg,
    pairs_ref,
    pcol_ref,
    prow_ref,
    xs_ref,
    pred_ref,
    slip_ref,
    green,
    wacc,
    got,
    series,
    resid,
    brow,
    send,
    part_a,
    part_b,
    gath_a,
    gath_b,
    full,
    s_x,
    r_x,
    s_p,
    r_pa,
    r_pb,
    s_g,
    r_ga,
    r_gb,
):
    n, reps, npix, npatch, parts, ifg_dev, lines = cfg
    me = lax.axis_index(("pix", "rep"))
    rep_size = lax.axis_size("rep")
    groups = npatch // LANES
    mine = me // reps
    gathered = n // reps

    def ident(d):
        return {"pix": d // rep_size, "rep": d % rep_size}

    def settle(buf, count, sem):
        view = buf.at[pl.ds(0, count)]
        pltpu.make_async_copy(view, view, sem).wait()

    barrier = pltpu.get_barrier_semaphore()

    @pl.loop(1, n)
    def _(k):
        pl.semaphore_signal(
            barrier, inc=1, device_id=ident((me + k) % n), device_id_type=pl.DeviceIdType.MESH
        )

    pl.semaphore_wait(barrier, n - 1)

    @pl.loop(1, n)
    def _(k):
        d = (me + k) % n
        pltpu.make_async_remote_copy(
            src_ref=xs_ref.at[d],
            dst_ref=got.at[me],
            send_sem=s_x,
            recv_sem=r_x.at[0],
            device_id=ident(d),
            device_id_type=pl.DeviceIdType.MESH,
        ).start()

    own_copy = pltpu.make_async_copy(xs_ref.at[me], got.at[me], r_x.at[1])
    own_copy.start()

    strip, wide = 32, 256
    per_line = IMG_W // strip

    for line in range(lines):

        @pl.loop(0, per_line)
        def _(t):
            start = pl.multiple_of(line * IMG_W + t * strip, strip)
            col = pcol_ref[pl.ds(start, strip), :]
            xpos = jnp.broadcast_to(col[:, 0:1], (strip, LANES))
            east = jnp.broadcast_to(col[:, 1:2], (strip, LANES))
            north = jnp.broadcast_to(col[:, 2:3], (strip, LANES))
            upward = jnp.broadcast_to(col[:, 3:4], (strip, LANES))
            total = jnp.zeros((strip, LANES), F32)
            for c in range(npatch // wide):
                halves = []
                for j in range(wide // LANES):
                    at = slice(c * wide + j * LANES, c * wide + (j + 1) * LANES)
                    u = (xpos - prow_ref[0:1, at]) * prow_ref[1:2, at]
                    r2 = u * u + prow_ref[4 + 2 * line : 5 + 2 * line, at]
                    inv = lax.rsqrt(r2)
                    num = east * u + north * prow_ref[3 + 2 * line : 4 + 2 * line, at]
                    num = num + upward * prow_ref[2:3, at]
                    g = num * (inv * inv * inv)
                    total = total + jnp.abs(g)
                    halves.append(g.astype(BF16))
                green[pl.ds(start, strip), c * wide : (c + 1) * wide] = jnp.concatenate(halves, 1)
            wacc[pl.ds(start, strip), :] = total

    weight = lax.dot_general(
        jnp.ones((EXTRA, LANES), F32),
        wacc[...],
        NT,
        precision=lax.Precision.HIGHEST,
        preferred_element_type=F32,
    ).astype(BF16)
    block = 512

    @pl.loop(0, npatch // block)
    def _(b):
        cols = pl.ds(pl.multiple_of(b * block, block), block)
        row = jnp.dot(weight, jnp.abs(green[:, cols]), preferred_element_type=F32)
        brow[:, cols] = row

    rows = parts * n * ifg_dev
    ep = lax.broadcasted_iota(jnp.int32, (NEP, rows), 0)
    later = (ep == pairs_ref[1:2, :]).astype(F32)
    earlier = (ep == pairs_ref[0:1, :]).astype(F32)
    design = later - earlier
    design_half = design.astype(BF16)
    sub = lax.broadcasted_iota(jnp.int32, (NEP, NEP), 0)
    lane = lax.broadcasted_iota(jnp.int32, (NEP, NEP), 1)
    normal = lax.dot_general(design_half, design_half, NT, preferred_element_type=F32) * (1.0 / parts)
    normal = normal + jnp.where(sub == lane, damping, 0.0)

    def sweep(k, m):
        col = jnp.sum(jnp.where(lane == k, m, 0.0), axis=1, keepdims=True)
        row = jnp.sum(jnp.where(sub == k, m, 0.0), axis=0, keepdims=True)
        pivot = jnp.sum(jnp.where(lane[0:1] == k, row, 0.0), axis=1, keepdims=True)
        inv = 1.0 / pivot
        scaled = row * inv
        new = m - col * scaled
        new = jnp.where(lane == k, col * inv, new)
        new = jnp.where(sub == k, scaled, new)
        return jnp.where((sub == k) & (lane == k), -inv, new)

    inverse = -lax.fori_loop(0, NEP, sweep, normal)
    inv_hi = inverse.astype(BF16)
    rest = inverse - inv_hi.astype(F32)
    inv_mid = rest.astype(BF16)
    inv_lo = (rest - inv_mid.astype(F32)).astype(BF16)
    pseudo = (
        jnp.dot(inv_hi, design_half, preferred_element_type=F32)
        + jnp.dot(inv_mid, design_half, preferred_element_type=F32)
        + jnp.dot(inv_lo, design_half, preferred_element_type=F32)
    )
    which = (lax.broadcasted_iota(jnp.int32, (NEP, rows), 1) // ifg_dev) % parts

    settle(got, n - 1, r_x.at[0])
    own_copy.wait()
    settle(got, n - 1, s_x)
    width = npix // parts
    stacked = got[...].reshape(rows, width)
    for h in range(parts):
        keep = jnp.where(which == h, pseudo, 0.0)
        hi = keep.astype(BF16)
        lo = (keep - hi.astype(F32)).astype(BF16)
        piece = jnp.dot(hi, stacked, preferred_element_type=F32)
        piece = piece + jnp.dot(lo, stacked, preferred_element_type=F32)
        series[:, h * width : (h + 1) * width] = piece
        resid[:, h * width : (h + 1) * width] = piece.astype(BF16)

    per_block = block // LANES
    blocks = npatch // block
    first_block = mine // per_block

    def project(part, recv_sem):
        @pl.loop(0, blocks)
        def _(b):
            at = (first_block + 1 + b) % blocks
            cols = pl.ds(pl.multiple_of(at * block, block), block)
            out = jnp.dot(resid[...], green[:, cols], preferred_element_type=F32)
            bound = brow[:, cols]
            high = bound.astype(BF16)
            low = (bound - high.astype(F32)).astype(BF16)
            pick = lax.broadcasted_iota(jnp.int32, (EXTRA, block), 0) == 0
            tail = jnp.where(pick, high.astype(F32), low.astype(F32)).astype(BF16)
            half = out.astype(BF16)
            for j in range(per_block):
                send[at * per_block + j, 0:NEP, :] = half[:, j * LANES : (j + 1) * LANES]
                send[at * per_block + j, NEP : NEP + EXTRA, :] = tail[:, j * LANES : (j + 1) * LANES]
            for j in range(per_block):
                group = at * per_block + j
                for r in range(reps):
                    d = group * reps + r

                    @pl.when(d != me)
                    def _():
                        pltpu.make_async_remote_copy(
                            src_ref=send.at[group],
                            dst_ref=part.at[me],
                            send_sem=s_p,
                            recv_sem=recv_sem,
                            device_id=ident(d),
                            device_id_type=pl.DeviceIdType.MESH,
                        ).start()

        part[me, :, :] = send[mine, :, :]
        settle(part, n - 1, recv_sem)
        settle(part, n - 1, s_p)
        return lax.fori_loop(
            1, n, lambda d, acc: acc + part[d].astype(F32), part[0].astype(F32)
        )

    def share(slip, gath, recv_sem):
        gath[mine, :, :] = slip.astype(BF16)

        @pl.loop(1, gathered)
        def _(k):
            d = (me + k * reps) % n
            pltpu.make_async_remote_copy(
                src_ref=gath.at[mine],
                dst_ref=gath.at[mine],
                send_sem=s_g,
                recv_sem=recv_sem,
                device_id=ident(d),
                device_id_type=pl.DeviceIdType.MESH,
            ).start()

        settle(gath, gathered - 1, recv_sem)
        settle(gath, gathered - 1, s_g)
        for g in range(groups):
            full[:, g * LANES : (g + 1) * LANES] = gath[g]

    tile = 512
    sums = project(part_a, r_pa)
    bound = sums[NEP : NEP + 1] + sums[NEP + 1 : NEP + 2]
    slip = sums[:NEP] / bound
    share(slip, gath_a, r_ga)

    @pl.loop(0, npix // tile)
    def _(t):
        at = pl.ds(pl.multiple_of(t * tile, tile), tile)
        guess = lax.dot_general(full[...], green[at, :], NT, preferred_element_type=F32)
        resid[:, at] = (series[:, at] - guess).astype(BF16)

    sums = project(part_b, r_pb)
    slip = slip + sums[:NEP] / bound
    slip_ref[...] = slip
    share(slip, gath_b, r_gb)

    @pl.loop(0, npix // tile)
    def _(t):
        at = pl.ds(pl.multiple_of(t * tile, tile), tile)
        pred_ref[:, at] = lax.dot_general(full[...], green[at, :], NT, preferred_element_type=F32)


def on_device(interferograms, epoch_pairs, los, patch_place, patch_depth):
    n = lax.axis_size(("pix", "rep"))
    me = lax.axis_index(("pix", "rep"))
    ifg_dev, total = interferograms.shape
    npix = total // n
    npatch = patch_depth.shape[0]
    own = npatch // n
    reps = max(LANES // own, 1)
    parts = max(16 // ifg_dev, 1)
    width = npix // parts
    lines = npix // IMG_W
    rows = parts * n * ifg_dev

    xs = interferograms.astype(BF16).reshape(ifg_dev, n, parts, width)
    xs = xs.transpose(1, 2, 0, 3).reshape(n, parts * ifg_dev, width)
    pairs = jnp.broadcast_to(
        epoch_pairs.reshape(2, n, 1, ifg_dev), (2, n, parts, ifg_dev)
    ).reshape(2, rows)

    column = (lax.iota(jnp.int32, npix) % IMG_W).astype(F32)
    xpos = (column + 0.5) * pixel_step
    pcol = jnp.concatenate([xpos[None], los], 0).T

    line = me * lines + lax.iota(jnp.int32, lines)
    ypos = (line.astype(F32) + 0.5) * pixel_step
    patch_x = (patch_place[0].astype(F32) + 0.5) * patch_step
    patch_y = (patch_place[1].astype(F32) + 0.5) * patch_step
    depth = depth_base + depth_step * patch_depth.astype(F32)
    scale = lax.rsqrt(depth)
    prows = [patch_x, scale, depth * scale]
    for i in range(lines):
        dy = ypos[i] - patch_y
        prows += [dy * scale, dy * dy / depth + depth]
    prow = jnp.stack(prows)

    groups = npatch // LANES
    cfg = (n, reps, npix, npatch, parts, ifg_dev, lines)
    vmem = pl.BlockSpec(memory_space=pltpu.VMEM)
    piece = (NEP + EXTRA, LANES)
    dma = pltpu.SemaphoreType.DMA
    predicted, slip = pl.pallas_call(
        functools.partial(kernel, cfg),
        out_shape=(
            jax.ShapeDtypeStruct((NEP, npix), F32),
            jax.ShapeDtypeStruct((NEP, LANES), F32),
        ),
        in_specs=[vmem, vmem, vmem, pl.BlockSpec(memory_space=pl.ANY)],
        out_specs=(vmem, vmem),
        scratch_shapes=[
            pltpu.VMEM((npix, npatch), BF16),
            pltpu.VMEM((npix, LANES), F32),
            pltpu.VMEM((n, parts * ifg_dev, width), BF16),
            pltpu.VMEM((NEP, npix), F32),
            pltpu.VMEM((NEP, npix), BF16),
            pltpu.VMEM((EXTRA, npatch), F32),
            pltpu.VMEM((groups,) + piece, BF16),
            pltpu.VMEM((n,) + piece, BF16),
            pltpu.VMEM((n,) + piece, BF16),
            pltpu.VMEM((groups, NEP, LANES), BF16),
            pltpu.VMEM((groups, NEP, LANES), BF16),
            pltpu.VMEM((NEP, npatch), BF16),
            dma,
            dma((2,)),
            dma,
            dma,
            dma,
            dma,
            dma,
            dma,
        ],
        compiler_params=pltpu.CompilerParams(
            collective_id=0, has_side_effects=True, vmem_limit_bytes=62 * 1024 * 1024
        ),
    )(pairs, pcol, prow, xs)
    if reps > 1:
        slip = lax.dynamic_slice_in_dim(slip, (me % reps) * own, own, 1)
    return (predicted, slip)


def solution(mesh):
    placed = (P(("pix", "rep"), None), P(), P(None, ("pix", "rep")), P(), P())
    return jax.shard_map(
        on_device,
        mesh=mesh,
        in_specs=placed,
        out_specs=(P(None, ("pix", "rep")), P(None, ("pix", "rep"))),
        check_vma=False,
    )
```

```python
import functools

import jax
import jax.numpy as jnp
from jax import lax
from jax.experimental import pallas as pl
from jax.experimental.pallas import tpu as pltpu
from jax.sharding import PartitionSpec as P

NEP = 64
IMG_W = 1024
LANES = 128

pixel_step = 0.1
patch_step = 0.4
damping = 0.5
depth_base = 0.5
depth_step = 0.25

F32 = jnp.float32
BF16 = jnp.bfloat16
NT = (((1,), (1,)), ((), ()))
EXTRA = 16


def kernel(
    cfg,
    pairs_ref,
    los_ref,
    place_ref,
    depth_ref,
    xs_ref,
    pred_ref,
    slip_ref,
    pcol_ref,
    prow_ref,
    mat,
    green,
    wacc,
    got,
    series,
    resid,
    bsend,
    bpart,
    send,
    part_a,
    part_b,
    gath_a,
    gath_b,
    full,
    guess,
    s_x,
    r_x,
    s_b,
    r_b,
    s_p,
    r_pa,
    r_pb,
    s_g,
    r_ga,
    r_gb,
):
    n, reps, npix, npatch, parts, ifg_dev, lines = cfg
    me = lax.axis_index(("pix", "rep"))
    rep_size = lax.axis_size("rep")
    groups = npatch // LANES
    mine = me // reps
    gathered = n // reps

    def ident(d):
        return {"pix": d // rep_size, "rep": d % rep_size}

    def settle(buf, count, sem):
        view = buf.at[pl.ds(0, count)]
        pltpu.make_async_copy(view, view, sem).wait()

    barrier = pltpu.get_barrier_semaphore()

    @pl.loop(1, n)
    def _(k):
        pl.semaphore_signal(
            barrier, inc=1, device_id=ident((me + k) % n), device_id_type=pl.DeviceIdType.MESH
        )

    pl.semaphore_wait(barrier, n - 1)

    @pl.loop(1, n)
    def _(k):
        d = (me + k) % n
        pltpu.make_async_remote_copy(
            src_ref=xs_ref.at[d],
            dst_ref=got.at[me],
            send_sem=s_x,
            recv_sem=r_x.at[0],
            device_id=ident(d),
            device_id_type=pl.DeviceIdType.MESH,
        ).start()

    own_copy = pltpu.make_async_copy(xs_ref.at[me], got.at[me], r_x.at[1])
    own_copy.start()

    patch_x = (place_ref[0:1, :].astype(F32) + 0.5) * patch_step
    patch_y = (place_ref[1:2, :].astype(F32) + 0.5) * patch_step
    depth = depth_base + depth_step * depth_ref[...].astype(F32)
    scale = lax.rsqrt(depth)
    prow_ref[0:1, :] = patch_x
    prow_ref[1:2, :] = scale
    prow_ref[2:3, :] = depth * scale
    for line in range(lines):
        dy = ((me * lines + line).astype(F32) + 0.5) * pixel_step - patch_y
        prow_ref[3 + 2 * line : 4 + 2 * line, :] = dy * scale
        prow_ref[4 + 2 * line : 5 + 2 * line, :] = dy * dy / depth + depth
    pcol_ref[...] = jnp.concatenate([los_ref[...], jnp.zeros((5, npix), F32)], 0).T

    rows = parts * n * ifg_dev
    nifg = n * ifg_dev
    ep = lax.broadcasted_iota(jnp.int32, (NEP, nifg), 0)
    later = (ep == pairs_ref[1:2, :]).astype(F32)
    earlier = (ep == pairs_ref[0:1, :]).astype(F32)
    design = (later - earlier).astype(BF16)
    slot = lax.broadcasted_iota(jnp.int32, (nifg, rows), 1)
    source = slot // (parts * ifg_dev) * ifg_dev + slot % ifg_dev
    spread = (lax.broadcasted_iota(jnp.int32, (nifg, rows), 0) == source).astype(F32).astype(BF16)
    design_half = jnp.dot(design, spread, preferred_element_type=F32).astype(BF16)
    sub = lax.broadcasted_iota(jnp.int32, (NEP, NEP), 0)
    lane = lax.broadcasted_iota(jnp.int32, (NEP, NEP), 1)
    normal = lax.dot_general(design, design, NT, preferred_element_type=F32)
    mat[...] = normal + jnp.where(sub == lane, damping, 0.0)

    def sweep(k):
        m = mat[...]
        col = jnp.sum(jnp.where(lane == k, m, 0.0), axis=1, keepdims=True)
        row = jnp.sum(jnp.where(sub == k, m, 0.0), axis=0, keepdims=True)
        pivot = jnp.sum(jnp.where(lane[0:1] == k, row, 0.0), axis=1, keepdims=True)
        inv = 1.0 / pivot
        scaled = row * inv
        new = m - col * scaled
        new = jnp.where(lane == k, col * inv, new)
        new = jnp.where(sub == k, scaled, new)
        mat[...] = jnp.where((sub == k) & (lane == k), -inv, new)

    strip, wide = 32, 256
    per_line = IMG_W // strip

    for line in range(lines):

        @pl.loop(0, per_line)
        def _(t):
            start = pl.multiple_of(line * IMG_W + t * strip, strip)
            col = pcol_ref[pl.ds(start, strip), :]
            cell = t * strip + lax.broadcasted_iota(jnp.int32, (strip, LANES), 0)
            xpos = (cell.astype(F32) + 0.5) * pixel_step
            east = jnp.broadcast_to(col[:, 0:1], (strip, LANES))
            north = jnp.broadcast_to(col[:, 1:2], (strip, LANES))
            upward = jnp.broadcast_to(col[:, 2:3], (strip, LANES))
            if (line + 1) * per_line <= NEP:
                sweep(line * per_line + t)
            total = jnp.zeros((strip, LANES), F32)
            for c in range(npatch // wide):
                halves = []
                for j in range(wide // LANES):
                    at = slice(c * wide + j * LANES, c * wide + (j + 1) * LANES)
                    u = (xpos - prow_ref[0:1, at]) * prow_ref[1:2, at]
                    r2 = u * u + prow_ref[4 + 2 * line : 5 + 2 * line, at]
                    inv = lax.rsqrt(r2)
                    num = east * u + north * prow_ref[3 + 2 * line : 4 + 2 * line, at]
                    num = num + upward * prow_ref[2:3, at]
                    g = num * (inv * inv * inv)
                    total = total + jnp.abs(g)
                    halves.append(g.astype(BF16))
                green[pl.ds(start, strip), c * wide : (c + 1) * wide] = jnp.concatenate(halves, 1)
            wacc[pl.ds(start, strip), :] = total

    weight = lax.dot_general(
        jnp.ones((EXTRA, LANES), F32),
        wacc[...],
        NT,
        precision=lax.Precision.HIGHEST,
        preferred_element_type=F32,
    ).astype(BF16)
    block = 512

    @pl.loop(0, npatch // block)
    def _(b):
        cols = pl.ds(pl.multiple_of(b * block, block), block)
        row = jnp.dot(weight, jnp.abs(green[:, cols]), preferred_element_type=F32)
        high = row.astype(BF16)
        low = (row - high.astype(F32)).astype(BF16)
        pick = lax.broadcasted_iota(jnp.int32, (EXTRA, block), 0) == 0
        tail = jnp.where(pick, high.astype(F32), low.astype(F32)).astype(BF16)
        for j in range(block // LANES):
            bsend[b * (block // LANES) + j, :, :] = tail[:, j * LANES : (j + 1) * LANES]

    @pl.loop(1, n)
    def _(k):
        d = (me + k) % n
        pltpu.make_async_remote_copy(
            src_ref=bsend.at[d // reps],
            dst_ref=bpart.at[me],
            send_sem=s_b,
            recv_sem=r_b,
            device_id=ident(d),
            device_id_type=pl.DeviceIdType.MESH,
        ).start()

    bpart[me, :, :] = bsend[mine, :, :]

    @pl.loop(min(lines, NEP // per_line) * per_line, NEP)
    def _(k):
        sweep(k)

    inverse = -mat[...]
    inv_hi = inverse.astype(BF16)
    rest = inverse - inv_hi.astype(F32)
    inv_mid = rest.astype(BF16)
    inv_lo = (rest - inv_mid.astype(F32)).astype(BF16)
    pseudo = (
        jnp.dot(inv_hi, design_half, preferred_element_type=F32)
        + jnp.dot(inv_mid, design_half, preferred_element_type=F32)
        + jnp.dot(inv_lo, design_half, preferred_element_type=F32)
    )
    which = (lax.broadcasted_iota(jnp.int32, (NEP, rows), 1) // ifg_dev) % parts

    settle(got, n - 1, r_x.at[0])
    own_copy.wait()
    settle(got, n - 1, s_x)
    width = npix // parts
    stacked = got[...].reshape(rows, width)
    for h in range(parts):
        keep = jnp.where(which == h, pseudo, 0.0)
        hi = keep.astype(BF16)
        lo = (keep - hi.astype(F32)).astype(BF16)
        piece = jnp.dot(hi, stacked, preferred_element_type=F32)
        piece = piece + jnp.dot(lo, stacked, preferred_element_type=F32)
        series[:, h * width : (h + 1) * width] = piece
        resid[:, h * width : (h + 1) * width] = piece.astype(BF16)

    per_block = block // LANES
    blocks = npatch // block
    first_block = mine // per_block

    def project(part, recv_sem, first):
        @pl.loop(0, blocks)
        def _(b):
            at = (first_block + 1 + b) % blocks
            cols = pl.ds(pl.multiple_of(at * block, block), block)
            out = jnp.dot(resid[...], green[:, cols], preferred_element_type=F32)
            half = out.astype(BF16)
            for j in range(per_block):
                send[at * per_block + j, :, :] = half[:, j * LANES : (j + 1) * LANES]
            for j in range(per_block):
                group = at * per_block + j
                for r in range(reps):
                    d = group * reps + r

                    @pl.when(d != me)
                    def _():
                        pltpu.make_async_remote_copy(
                            src_ref=send.at[group],
                            dst_ref=part.at[me],
                            send_sem=s_p,
                            recv_sem=recv_sem,
                            device_id=ident(d),
                            device_id_type=pl.DeviceIdType.MESH,
                        ).start()

        part[me, :, :] = send[mine, :, :]
        settle(part, n - 1, recv_sem)
        settle(part, n - 1, s_p)
        bound = None
        if first:
            settle(bpart, n - 1, r_b)
            settle(bpart, n - 1, s_b)
            both = lax.fori_loop(
                1, n, lambda d, acc: acc + bpart[d].astype(F32), bpart[0].astype(F32)
            )
            bound = both[0:1] + both[1:2]
        total = lax.fori_loop(
            1, n, lambda d, acc: acc + part[d].astype(F32), part[0].astype(F32)
        )
        return total, bound

    tile = 512

    def share(slip, gath, recv_sem, target):
        gath[mine, :, :] = slip.astype(BF16)

        @pl.loop(1, gathered)
        def _(k):
            d = (me + (n - k * reps)) % n
            pltpu.make_async_remote_copy(
                src_ref=gath.at[mine],
                dst_ref=gath.at[mine],
                send_sem=s_g,
                recv_sem=recv_sem.at[first_block],
                device_id=ident(d),
                device_id_type=pl.DeviceIdType.MESH,
            ).start()

        for i in range(blocks):
            at = (first_block + i) % blocks
            settle(gath, per_block - 1 if i == 0 else per_block, recv_sem.at[at])
            for j in range(per_block):
                full[:, j * LANES : (j + 1) * LANES] = gath[at * per_block + j]
            cols = pl.ds(pl.multiple_of(at * block, block), block)

            @pl.loop(0, npix // tile)
            def _(t):
                here = pl.ds(pl.multiple_of(t * tile, tile), tile)
                out = lax.dot_general(full[...], green[here, cols], NT, preferred_element_type=F32)
                if i > 0:
                    out = target[:, here] + out
                target[:, here] = out

        settle(gath, gathered - 1, s_g)

    sums, bound = project(part_a, r_pa, True)
    slip = sums / bound
    share(slip, gath_a, r_ga, guess)
    resid[...] = (series[...] - guess[...]).astype(BF16)
    slip = slip + project(part_b, r_pb, False)[0] / bound
    slip_ref[...] = slip
    share(slip, gath_b, r_gb, pred_ref)


def on_device(interferograms, epoch_pairs, los, patch_place, patch_depth):
    n = lax.axis_size(("pix", "rep"))
    me = lax.axis_index(("pix", "rep"))
    ifg_dev, total = interferograms.shape
    npix = total // n
    npatch = patch_depth.shape[0]
    own = npatch // n
    reps = max(LANES // own, 1)
    parts = max(16 // ifg_dev, 1)
    width = npix // parts
    lines = npix // IMG_W

    xs = interferograms.astype(BF16).reshape(ifg_dev, n, parts, width)
    xs = xs.transpose(1, 2, 0, 3).reshape(n, parts * ifg_dev, width)
    groups = npatch // LANES
    cfg = (n, reps, npix, npatch, parts, ifg_dev, lines)
    vmem = pl.BlockSpec(memory_space=pltpu.VMEM)
    piece = (NEP, LANES)
    block = 512
    dma = pltpu.SemaphoreType.DMA
    predicted, slip = pl.pallas_call(
        functools.partial(kernel, cfg),
        out_shape=(
            jax.ShapeDtypeStruct((NEP, npix), F32),
            jax.ShapeDtypeStruct((NEP, LANES), F32),
        ),
        in_specs=[vmem, vmem, vmem, vmem, pl.BlockSpec(memory_space=pl.ANY)],
        out_specs=(vmem, vmem),
        scratch_shapes=[
            pltpu.VMEM((npix, 8), F32),
            pltpu.VMEM((3 + 2 * lines, npatch), F32),
            pltpu.VMEM((NEP, NEP), F32),
            pltpu.VMEM((npix, npatch), BF16),
            pltpu.VMEM((npix, LANES), F32),
            pltpu.VMEM((n, parts * ifg_dev, width), BF16),
            pltpu.VMEM((NEP, npix), F32),
            pltpu.VMEM((NEP, npix), BF16),
            pltpu.VMEM((groups, EXTRA, LANES), BF16),
            pltpu.VMEM((n, EXTRA, LANES), BF16),
            pltpu.VMEM((groups,) + piece, BF16),
            pltpu.VMEM((n,) + piece, BF16),
            pltpu.VMEM((n,) + piece, BF16),
            pltpu.VMEM((groups, NEP, LANES), BF16),
            pltpu.VMEM((groups, NEP, LANES), BF16),
            pltpu.VMEM((NEP, block), BF16),
            pltpu.VMEM((NEP, npix), F32),
            dma,
            dma((2,)),
            dma,
            dma,
            dma,
            dma,
            dma,
            dma,
            dma((npatch // block,)),
            dma((npatch // block,)),
        ],
        compiler_params=pltpu.CompilerParams(
            collective_id=0, has_side_effects=True, vmem_limit_bytes=62 * 1024 * 1024
        ),
    )(epoch_pairs, los, patch_place, patch_depth[None], xs)
    if reps > 1:
        slip = lax.dynamic_slice_in_dim(slip, (me % reps) * own, own, 1)
    return (predicted, slip)


def solution(mesh):
    placed = (P(("pix", "rep"), None), P(), P(None, ("pix", "rep")), P(), P())
    return jax.shard_map(
        on_device,
        mesh=mesh,
        in_specs=placed,
        out_specs=(P(None, ("pix", "rep")), P(None, ("pix", "rep"))),
        check_vma=False,
    )
```

```python
import functools

import jax
import jax.numpy as jnp
from jax import lax
from jax.experimental import pallas as pl
from jax.experimental.pallas import tpu as pltpu
from jax.sharding import PartitionSpec as P

NEP = 64
IMG_W = 1024
LANES = 128

pixel_step = 0.1
patch_step = 0.4
damping = 0.5
depth_base = 0.5
depth_step = 0.25

F32 = jnp.float32
BF16 = jnp.bfloat16
NT = (((1,), (1,)), ((), ()))
EXTRA = 16


def kernel(
    cfg,
    pairs_ref,
    los_ref,
    place_ref,
    depth_ref,
    xs_ref,
    pred_ref,
    slip_ref,
    pcol_ref,
    prow_ref,
    mat,
    green,
    wacc,
    got,
    series,
    resid,
    bsend,
    bpart,
    send,
    part_a,
    part_b,
    gath_a,
    gath_b,
    full,
    guess,
    s_x,
    r_x,
    s_b,
    r_b,
    s_p,
    r_pa,
    r_pb,
    s_g,
    r_ga,
    r_gb,
):
    n, reps, npix, npatch, parts, ifg_dev, lines = cfg
    me = lax.axis_index(("pix", "rep"))
    rep_size = lax.axis_size("rep")
    groups = npatch // LANES
    mine = me // reps
    gathered = n // reps

    def ident(d):
        return {"pix": d // rep_size, "rep": d % rep_size}

    def settle(buf, count, sem):
        view = buf.at[pl.ds(0, count)]
        pltpu.make_async_copy(view, view, sem).wait()

    barrier = pltpu.get_barrier_semaphore()

    @pl.loop(1, n)
    def _(k):
        pl.semaphore_signal(
            barrier, inc=1, device_id=ident((me + k) % n), device_id_type=pl.DeviceIdType.MESH
        )

    pl.semaphore_wait(barrier, n - 1)

    @pl.loop(1, n)
    def _(k):
        d = (me + k) % n
        pltpu.make_async_remote_copy(
            src_ref=xs_ref.at[d],
            dst_ref=got.at[me],
            send_sem=s_x,
            recv_sem=r_x.at[0],
            device_id=ident(d),
            device_id_type=pl.DeviceIdType.MESH,
        ).start()

    own_copy = pltpu.make_async_copy(xs_ref.at[me], got.at[me], r_x.at[1])
    own_copy.start()

    patch_x = (place_ref[0:1, :].astype(F32) + 0.5) * patch_step
    patch_y = (place_ref[1:2, :].astype(F32) + 0.5) * patch_step
    depth = depth_base + depth_step * depth_ref[...].astype(F32)
    scale = lax.rsqrt(depth)
    prow_ref[0:1, :] = patch_x
    prow_ref[1:2, :] = scale
    prow_ref[2:3, :] = depth * scale
    for line in range(lines):
        dy = ((me * lines + line).astype(F32) + 0.5) * pixel_step - patch_y
        prow_ref[3 + 2 * line : 4 + 2 * line, :] = dy * scale
        prow_ref[4 + 2 * line : 5 + 2 * line, :] = dy * dy / depth + depth
    pcol_ref[...] = jnp.concatenate([los_ref[...], jnp.zeros((5, npix), F32)], 0).T

    rows = parts * n * ifg_dev
    nifg = n * ifg_dev
    ep = lax.broadcasted_iota(jnp.int32, (NEP, nifg), 0)
    later = (ep == pairs_ref[1:2, :]).astype(F32)
    earlier = (ep == pairs_ref[0:1, :]).astype(F32)
    design = (later - earlier).astype(BF16)
    slot = lax.broadcasted_iota(jnp.int32, (nifg, rows), 1)
    source = slot // (parts * ifg_dev) * ifg_dev + slot % ifg_dev
    spread = (lax.broadcasted_iota(jnp.int32, (nifg, rows), 0) == source).astype(F32).astype(BF16)
    design_half = jnp.dot(design, spread, preferred_element_type=F32).astype(BF16)
    sub = lax.broadcasted_iota(jnp.int32, (NEP, NEP), 0)
    lane = lax.broadcasted_iota(jnp.int32, (NEP, NEP), 1)
    normal = lax.dot_general(design, design, NT, preferred_element_type=F32)
    mat[...] = normal + jnp.where(sub == lane, damping, 0.0)

    def sweep(k):
        m = mat[...]
        col = jnp.sum(jnp.where(lane == k, m, 0.0), axis=1, keepdims=True)
        row = jnp.sum(jnp.where(sub == k, m, 0.0), axis=0, keepdims=True)
        pivot = jnp.sum(jnp.where(lane[0:1] == k, row, 0.0), axis=1, keepdims=True)
        inv = 1.0 / pivot
        scaled = row * inv
        new = m - col * scaled
        new = jnp.where(lane == k, col * inv, new)
        new = jnp.where(sub == k, scaled, new)
        mat[...] = jnp.where((sub == k) & (lane == k), -inv, new)

    strip, wide = 32, 256
    per_line = IMG_W // strip

    for line in range(lines):

        @pl.loop(0, per_line)
        def _(t):
            start = pl.multiple_of(line * IMG_W + t * strip, strip)
            col = pcol_ref[pl.ds(start, strip), :]
            cell = t * strip + lax.broadcasted_iota(jnp.int32, (strip, LANES), 0)
            xpos = (cell.astype(F32) + 0.5) * pixel_step
            east = jnp.broadcast_to(col[:, 0:1], (strip, LANES))
            north = jnp.broadcast_to(col[:, 1:2], (strip, LANES))
            upward = jnp.broadcast_to(col[:, 2:3], (strip, LANES))
            if (line + 1) * per_line <= NEP:
                sweep(line * per_line + t)
            total = jnp.zeros((strip, LANES), F32)
            for c in range(npatch // wide):
                halves = []
                for j in range(wide // LANES):
                    at = slice(c * wide + j * LANES, c * wide + (j + 1) * LANES)
                    u = (xpos - prow_ref[0:1, at]) * prow_ref[1:2, at]
                    r2 = u * u + prow_ref[4 + 2 * line : 5 + 2 * line, at]
                    inv = lax.rsqrt(r2)
                    num = east * u + north * prow_ref[3 + 2 * line : 4 + 2 * line, at]
                    num = num + upward * prow_ref[2:3, at]
                    g = num * (inv * inv * inv)
                    total = total + jnp.abs(g)
                    halves.append(g.astype(BF16))
                green[pl.ds(start, strip), c * wide : (c + 1) * wide] = jnp.concatenate(halves, 1)
            wacc[pl.ds(start, strip), :] = total

    weight = lax.dot_general(
        jnp.ones((EXTRA, LANES), F32),
        wacc[...],
        NT,
        precision=lax.Precision.HIGHEST,
        preferred_element_type=F32,
    ).astype(BF16)
    block = 512

    @pl.loop(0, npatch // block)
    def _(b):
        cols = pl.ds(pl.multiple_of(b * block, block), block)
        row = jnp.dot(weight, jnp.abs(green[:, cols]), preferred_element_type=F32)
        high = row.astype(BF16)
        low = (row - high.astype(F32)).astype(BF16)
        pick = lax.broadcasted_iota(jnp.int32, (EXTRA, block), 0) == 0
        tail = jnp.where(pick, high.astype(F32), low.astype(F32)).astype(BF16)
        for j in range(block // LANES):
            bsend[b * (block // LANES) + j, :, :] = tail[:, j * LANES : (j + 1) * LANES]

    @pl.loop(1, n)
    def _(k):
        d = (me + k) % n
        pltpu.make_async_remote_copy(
            src_ref=bsend.at[d // reps],
            dst_ref=bpart.at[me],
            send_sem=s_b,
            recv_sem=r_b,
            device_id=ident(d),
            device_id_type=pl.DeviceIdType.MESH,
        ).start()

    bpart[me, :, :] = bsend[mine, :, :]

    @pl.loop(min(lines, NEP // per_line) * per_line, NEP)
    def _(k):
        sweep(k)

    inverse = -mat[...]
    inv_hi = inverse.astype(BF16)
    rest = inverse - inv_hi.astype(F32)
    inv_mid = rest.astype(BF16)
    inv_lo = (rest - inv_mid.astype(F32)).astype(BF16)
    pseudo = (
        jnp.dot(inv_hi, design_half, preferred_element_type=F32)
        + jnp.dot(inv_mid, design_half, preferred_element_type=F32)
        + jnp.dot(inv_lo, design_half, preferred_element_type=F32)
    )
    which = (lax.broadcasted_iota(jnp.int32, (NEP, rows), 1) // ifg_dev) % parts

    settle(got, n - 1, r_x.at[0])
    own_copy.wait()
    settle(got, n - 1, s_x)
    width = npix // parts
    stacked = got[...].reshape(rows, width)
    for h in range(parts):
        keep = jnp.where(which == h, pseudo, 0.0)
        hi = keep.astype(BF16)
        lo = (keep - hi.astype(F32)).astype(BF16)
        piece = jnp.dot(hi, stacked, preferred_element_type=F32)
        piece = piece + jnp.dot(lo, stacked, preferred_element_type=F32)
        series[:, h * width : (h + 1) * width] = piece
        resid[:, h * width : (h + 1) * width] = piece.astype(BF16)

    per_block = block // LANES
    blocks = npatch // block
    first_block = mine // per_block
    side = blocks // 2

    def project(part, recv_sem, first):
        @pl.loop(0, blocks)
        def _(b):
            at = (first_block // side + 1 + b // side) % 2 * side + (first_block + 1 + b) % side
            cols = pl.ds(pl.multiple_of(at * block, block), block)
            out = jnp.dot(resid[...], green[:, cols], preferred_element_type=F32)
            half = out.astype(BF16)
            for j in range(per_block):
                send[at * per_block + j, :, :] = half[:, j * LANES : (j + 1) * LANES]
            for j in range(per_block):
                group = at * per_block + j
                for r in range(reps):
                    d = group * reps + r

                    @pl.when(d != me)
                    def _():
                        pltpu.make_async_remote_copy(
                            src_ref=send.at[group],
                            dst_ref=part.at[me],
                            send_sem=s_p,
                            recv_sem=recv_sem,
                            device_id=ident(d),
                            device_id_type=pl.DeviceIdType.MESH,
                        ).start()

        part[me, :, :] = send[mine, :, :]
        settle(part, n - 1, recv_sem)
        settle(part, n - 1, s_p)
        bound = None
        if first:
            settle(bpart, n - 1, r_b)
            settle(bpart, n - 1, s_b)
            both = lax.fori_loop(
                1, n, lambda d, acc: acc + bpart[d].astype(F32), bpart[0].astype(F32)
            )
            bound = both[0:1] + both[1:2]
        total = lax.fori_loop(
            1, n, lambda d, acc: acc + part[d].astype(F32), part[0].astype(F32)
        )
        return total, bound

    tile = 512

    def share(slip, gath, recv_sem, target):
        gath[mine, :, :] = slip.astype(BF16)

        @pl.loop(1, gathered)
        def _(k):
            d = (me + (n - k * reps)) % n
            pltpu.make_async_remote_copy(
                src_ref=gath.at[mine],
                dst_ref=gath.at[mine],
                send_sem=s_g,
                recv_sem=recv_sem.at[first_block],
                device_id=ident(d),
                device_id_type=pl.DeviceIdType.MESH,
            ).start()

        for i in range(blocks):
            at = (first_block + i) % blocks
            settle(gath, per_block - 1 if i == 0 else per_block, recv_sem.at[at])
            for j in range(per_block):
                full[:, j * LANES : (j + 1) * LANES] = gath[at * per_block + j]
            cols = pl.ds(pl.multiple_of(at * block, block), block)

            @pl.loop(0, npix // tile)
            def _(t):
                here = pl.ds(pl.multiple_of(t * tile, tile), tile)
                out = lax.dot_general(full[...], green[here, cols], NT, preferred_element_type=F32)
                if i > 0:
                    out = target[:, here] + out
                target[:, here] = out

        settle(gath, gathered - 1, s_g)

    sums, bound = project(part_a, r_pa, True)
    slip = sums / bound
    share(slip, gath_a, r_ga, guess)
    resid[...] = (series[...] - guess[...]).astype(BF16)
    slip = slip + project(part_b, r_pb, False)[0] / bound
    slip_ref[...] = slip
    share(slip, gath_b, r_gb, pred_ref)


def on_device(interferograms, epoch_pairs, los, patch_place, patch_depth):
    n = lax.axis_size(("pix", "rep"))
    me = lax.axis_index(("pix", "rep"))
    ifg_dev, total = interferograms.shape
    npix = total // n
    npatch = patch_depth.shape[0]
    own = npatch // n
    reps = max(LANES // own, 1)
    parts = max(16 // ifg_dev, 1)
    width = npix // parts
    lines = npix // IMG_W

    xs = interferograms.astype(BF16).reshape(ifg_dev, n, parts, width)
    xs = xs.transpose(1, 2, 0, 3).reshape(n, parts * ifg_dev, width)
    groups = npatch // LANES
    cfg = (n, reps, npix, npatch, parts, ifg_dev, lines)
    vmem = pl.BlockSpec(memory_space=pltpu.VMEM)
    piece = (NEP, LANES)
    block = 512
    dma = pltpu.SemaphoreType.DMA
    predicted, slip = pl.pallas_call(
        functools.partial(kernel, cfg),
        out_shape=(
            jax.ShapeDtypeStruct((NEP, npix), F32),
            jax.ShapeDtypeStruct((NEP, LANES), F32),
        ),
        in_specs=[vmem, vmem, vmem, vmem, pl.BlockSpec(memory_space=pl.ANY)],
        out_specs=(vmem, vmem),
        scratch_shapes=[
            pltpu.VMEM((npix, 8), F32),
            pltpu.VMEM((3 + 2 * lines, npatch), F32),
            pltpu.VMEM((NEP, NEP), F32),
            pltpu.VMEM((npix, npatch), BF16),
            pltpu.VMEM((npix, LANES), F32),
            pltpu.VMEM((n, parts * ifg_dev, width), BF16),
            pltpu.VMEM((NEP, npix), F32),
            pltpu.VMEM((NEP, npix), BF16),
            pltpu.VMEM((groups, EXTRA, LANES), BF16),
            pltpu.VMEM((n, EXTRA, LANES), BF16),
            pltpu.VMEM((groups,) + piece, BF16),
            pltpu.VMEM((n,) + piece, BF16),
            pltpu.VMEM((n,) + piece, BF16),
            pltpu.VMEM((groups, NEP, LANES), BF16),
            pltpu.VMEM((groups, NEP, LANES), BF16),
            pltpu.VMEM((NEP, block), BF16),
            pltpu.VMEM((NEP, npix), F32),
            dma,
            dma((2,)),
            dma,
            dma,
            dma,
            dma,
            dma,
            dma,
            dma((npatch // block,)),
            dma((npatch // block,)),
        ],
        compiler_params=pltpu.CompilerParams(
            collective_id=0, has_side_effects=True, vmem_limit_bytes=62 * 1024 * 1024
        ),
    )(epoch_pairs, los, patch_place, patch_depth[None], xs)
    if reps > 1:
        slip = lax.dynamic_slice_in_dim(slip, (me % reps) * own, own, 1)
    return (predicted, slip)


def solution(mesh):
    placed = (P(("pix", "rep"), None), P(), P(None, ("pix", "rep")), P(), P())
    return jax.shard_map(
        on_device,
        mesh=mesh,
        in_specs=placed,
        out_specs=(P(None, ("pix", "rep")), P(None, ("pix", "rep"))),
        check_vma=False,
    )
```
